32 devices in a mesh: dp: 2 (over x), expert: 16 (over z, y, core).
Axes of the slice: x: 2, y: 2, z: 4, core: 2. Of those that a mesh axis runs over, the one named last changes fastest.
Arguments:
- tokens: bfloat16 [32, 256, 1280], P(('dp', 'expert')), may hold values from -12 to 12
- router: bfloat16 [1280, 16], replicated, may hold values from -3 to 3
- w_in: bfloat16 [16, 1280, 5120], P('expert', None, 'dp'), may hold values from -0.15625 to 0.15625
- b_in: bfloat16 [16, 5120], P('expert'), may hold values from -3 to 3
- w_out: bfloat16 [16, 5120, 1280], P('expert', 'dp'), may hold values from -0.078125 to 0.078125
- b_out: bfloat16 [16, 1280], P('expert'), may hold values from -3 to 3
Outputs:
- mixed: bfloat16 [32, 256, 1280], P(('dp', 'expert'))
The draws below stay inside these ranges and needn't reach their ends.
All inputs are finite; a program needn't handle non-finite values.
Results may differ from the reference program's by a relative error of at most 0.014.
Values may be sent and summed in bfloat16 or wider, within the bound.
A program may use at most 64 MiB of HBM per device.

```python
import math
import jax
import jax.numpy as jnp
from jax import lax

D = 1280
HID = 5120
M = 256
EXPERTS = 16
IMAGES = 32


def image_tokens(base, index):
    image_key = jax.random.fold_in(base, index)
    values = jnp.clip(jax.random.normal(jax.random.fold_in(image_key, 1), (M, D), jnp.float32), -6.0, 6.0)
    return values


def draw_tokens(key, part):
    base = jax.random.fold_in(key, 11)
    stacked = jax.vmap(lambda index: image_tokens(base, index))(jnp.arange(IMAGES))
    return stacked.astype(jnp.bfloat16)


def draw_router(key, part):
    values = jax.random.normal(jax.random.fold_in(key, 12), (D, EXPERTS), jnp.float32) * (2.5 / math.sqrt(D))
    values = jnp.clip(values, -0.5, 0.5)
    return values.astype(jnp.bfloat16)


def shard_levels(key, dims, cuts, low, top_value):
    def one(dim, parts):
        draws = jax.random.uniform(jax.random.fold_in(jax.random.fold_in(key, 6), dim), (parts,), jnp.float32, low / len(cuts), top_value / len(cuts))
        return jnp.repeat(jnp.exp(draws), dims[dim] // parts).reshape((-1,) + (1,) * (len(dims) - dim - 1))

    gain = one(*cuts[0])
    for cut in cuts[1:]:
        gain = gain * one(*cut)
    return gain


def bell_draw(stream_key, dims, deviation, reach, cuts=(), dtype=jnp.bfloat16):
    factor_of = shard_levels(stream_key, dims, cuts, -0.22, 0.18) if cuts else 1.0
    array = jax.random.normal(stream_key, dims, jnp.float32) * deviation * factor_of
    return jnp.minimum(jnp.maximum(array, -reach), reach).astype(dtype)


def setup_inputs(seed: int = 0) -> dict:
    splits = jax.random.split(jax.random.key(seed), 7)
    tokens = draw_tokens(jax.random.fold_in(splits[6], 71), 0)
    router = draw_router(jax.random.fold_in(splits[6], 71), 0)
    w_in = bell_draw(splits[2], (EXPERTS, D, HID), D ** -0.5, 0.15625, ((0, 16), (2, 2)))
    b_in = bell_draw(splits[3], (EXPERTS, HID), 0.5, 3.0, ((0, 16),))
    w_out = bell_draw(splits[4], (EXPERTS, HID, D), HID ** -0.5, 0.078125, ((0, 16), (1, 2)))
    b_out = bell_draw(splits[5], (EXPERTS, D), 0.5, 3.0, ((0, 16),))
    return {"tokens": tokens, "router": router, "w_in": w_in, "b_in": b_in, "w_out": w_out, "b_out": b_out}


def run_expert(packed):
    slot_rows, weight_in, bias_in, weight_out, bias_out = packed
    hidden = jax.nn.gelu(jnp.dot(slot_rows, weight_in, preferred_element_type=jnp.float32) + bias_in.astype(jnp.float32), approximate=False).astype(jnp.bfloat16)
    return (jnp.dot(hidden, weight_out, preferred_element_type=jnp.float32) + bias_out.astype(jnp.float32)).astype(jnp.bfloat16)


def reference(tokens, router, w_in, b_in, w_out, b_out):
    logits = jnp.einsum("bmd,de->bme", tokens.astype(jnp.float32), router.astype(jnp.float32))
    dispatch = jax.nn.softmax(logits, axis=1).astype(jnp.bfloat16)
    combine = jax.nn.softmax(logits, axis=2).astype(jnp.bfloat16)
    slots = jnp.einsum("bme,bmd->ebd", dispatch.astype(jnp.float32), tokens.astype(jnp.float32)).astype(jnp.bfloat16)
    expert_out = lax.map(run_expert, (slots, w_in, b_in, w_out, b_out))
    mixed = jnp.einsum("bme,ebd->bmd", combine.astype(jnp.float32), expert_out.astype(jnp.float32))
    return mixed.astype(jnp.bfloat16)
```

```python
import functools

import jax
import jax.numpy as jnp
from jax import lax
from jax.experimental import pallas as pl
from jax.experimental.pallas import tpu as pltpu
from jax.sharding import PartitionSpec as P

MESH = pl.DeviceIdType.MESH
LANES = 128
SUBLANES = 16


def gelu(v):
    return v * (1.0 + lax.erf(v * (0.5**0.5))) * 0.5


def exchange(n, n_ex, me, source, row_of, landing, send_sem, recv_sem):
    def step(k, carry):
        dest = lax.rem(me + k, n)
        pltpu.make_async_remote_copy(
            src_ref=source.at[row_of(dest)],
            dst_ref=landing.at[me],
            send_sem=send_sem,
            recv_sem=recv_sem,
            device_id=(dest // n_ex, lax.rem(dest, n_ex)),
            device_id_type=MESH,
        ).start()
        return carry

    lax.fori_loop(1, n, step, 0)
    landing[me] = source[row_of(me)]


def wait_bytes(buffer, count, sem):
    rows = buffer.at[pl.ds(0, count)]
    pltpu.make_async_copy(rows, rows, sem).wait()


def kernel(
    n_dp,
    n_ex,
    tokens_hbm,
    router_hbm,
    w_in_hbm,
    b_in_hbm,
    w_out_hbm,
    b_out_hbm,
    out_ref,
    tok,
    router,
    w_in,
    b_in,
    w_out,
    b_out,
    wide_slots,
    wide_rows,
    send1,
    recv1,
    send2,
    recv2,
    x_ref,
    hid,
    comb_ref,
    eo,
    load_sems,
    w_in_sems,
    w_out_sems,
    send_sems,
    recv_sems,
):
    n = n_dp * n_ex
    me_dp = lax.axis_index("dp")
    me_ex = lax.axis_index("expert")
    me = me_dp * n_ex + me_ex
    width = tok.shape[1]
    chunks = width // LANES
    pitch = send1.shape[1]

    loads = [
        pltpu.make_async_copy(tokens_hbm.at[0], tok, load_sems.at[0]),
        pltpu.make_async_copy(router_hbm, router, load_sems.at[1]),
        pltpu.make_async_copy(b_in_hbm, b_in, load_sems.at[2]),
        pltpu.make_async_copy(b_out_hbm, b_out, load_sems.at[3]),
    ]
    for load in loads:
        load.start()

    barrier = pltpu.get_barrier_semaphore()

    def greet(k, carry):
        dest = lax.rem(me + k, n)
        pl.semaphore_signal(
            barrier, inc=1, device_id=(dest // n_ex, lax.rem(dest, n_ex)), device_id_type=MESH
        )
        return carry

    lax.fori_loop(1, n, greet, 0)

    def pieces(hbm, vmem, sems):
        count = sems.shape[0]
        rows = vmem.shape[0] // count
        return [
            pltpu.make_async_copy(
                hbm.at[0, pl.ds(i * rows, rows)], vmem.at[pl.ds(i * rows, rows)], sems.at[i]
            )
            for i in range(count)
        ]

    w_in_loads = pieces(w_in_hbm, w_in, w_in_sems)
    w_out_loads = pieces(w_out_hbm, w_out, w_out_sems)
    for load in w_in_loads + w_out_loads:
        load.start()

    loads[0].wait()
    loads[1].wait()
    logits = lax.dot_general(
        router[...], tok[...], (((1,), (1,)), ((), ())), preferred_element_type=jnp.float32
    )
    over_tokens = jnp.exp(logits - jnp.max(logits, axis=1, keepdims=True))
    dispatch = (over_tokens / jnp.sum(over_tokens, axis=1, keepdims=True)).astype(jnp.bfloat16)
    slots = jnp.dot(dispatch, tok[...], preferred_element_type=jnp.float32)
    for j in range(chunks):
        wide_slots[pl.ds(j, n_ex, stride=pitch), :] = slots[:, j * LANES : (j + 1) * LANES]
    send1[...] = wide_slots[...].reshape(send1.shape).astype(jnp.bfloat16)

    pl.semaphore_wait(barrier, n - 1)
    exchange(n, n_ex, me, send1, lambda d: lax.rem(d, n_ex), recv1, send_sems.at[0], recv_sems.at[0])

    over_experts = jnp.exp(logits - jnp.max(logits, axis=0, keepdims=True))
    combine = over_experts / jnp.sum(over_experts, axis=0, keepdims=True)
    comb_ref[...] = combine.astype(jnp.bfloat16)

    for load in loads[2:] + w_in_loads:
        load.wait()
    wait_bytes(recv1, n - 1, recv_sems.at[0])
    wide_rows[...] = recv1[...].astype(jnp.float32).reshape(wide_rows.shape)
    for j in range(chunks):
        x_ref[:, j * LANES : (j + 1) * LANES] = wide_rows[pl.ds(j, n, stride=pitch), :].astype(jnp.bfloat16)

    half = w_in.shape[1]
    tile = 2 * LANES

    @pl.loop(0, half // tile)
    def _(t):
        at = pl.multiple_of(t * tile, tile)
        bias = b_in[:, pl.ds(pl.multiple_of(me_dp * half + at, LANES), tile)].astype(jnp.float32)
        v = jnp.dot(x_ref[...], w_in[:, pl.ds(at, tile)], preferred_element_type=jnp.float32) + bias
        hid[:, pl.ds(at, tile)] = gelu(v).astype(jnp.bfloat16)

    for load in w_out_loads:
        load.wait()
    keep = (me_dp == 0).astype(jnp.float32)
    for at in range(0, width, tile):
        y = jnp.dot(hid[...], w_out[:, at : at + tile], preferred_element_type=jnp.float32)
        y = y + keep * b_out[:, at : at + tile].astype(jnp.float32)
        for c in range(tile // LANES):
            wide_rows[pl.ds(at // LANES + c, n, stride=pitch), :] = y[:, c * LANES : (c + 1) * LANES]
    send2[...] = wide_rows[...].reshape(send2.shape).astype(jnp.bfloat16)

    exchange(n, n_ex, me, send2, lambda d: d, recv2, send_sems.at[1], recv_sems.at[1])
    wait_bytes(recv2, n - 1, recv_sems.at[1])
    wide_rows[...] = recv2[...].astype(jnp.float32).reshape(wide_rows.shape)
    for j in range(chunks):
        total = wide_rows[pl.ds(j, n_ex, stride=pitch), :]
        for a in range(1, n_dp):
            total = total + wide_rows[pl.ds(a * n_ex * pitch + j, n_ex, stride=pitch), :]
        eo[:, j * LANES : (j + 1) * LANES] = total.astype(jnp.bfloat16)
    mixed = lax.dot_general(
        comb_ref[...], eo[...], (((0,), (0,)), ((), ())), preferred_element_type=jnp.float32
    )
    out_ref[0] = mixed.astype(jnp.bfloat16)
    wait_bytes(recv1, n - 1, send_sems.at[0])
    wait_bytes(recv2, n - 1, send_sems.at[1])


def shards(n_dp, n_ex, tokens, router, w_in, b_in, w_out, b_out):
    n = n_dp * n_ex
    images, m, width = tokens.shape
    assert images == 1 and w_in.shape[0] == 1
    half = w_in.shape[2]
    chunks = width // LANES
    pitch = -(-chunks // SUBLANES) * SUBLANES
    bf16, f32 = jnp.bfloat16, jnp.float32
    return pl.pallas_call(
        functools.partial(kernel, n_dp, n_ex),
        out_shape=jax.ShapeDtypeStruct(tokens.shape, bf16),
        in_specs=[pl.BlockSpec(memory_space=pltpu.HBM)] * 6,
        out_specs=pl.BlockSpec(memory_space=pltpu.VMEM),
        scratch_shapes=[
            pltpu.VMEM((m, width), bf16),
            pltpu.VMEM(router.shape[::-1], bf16),
            pltpu.VMEM(w_in.shape[1:], bf16),
            pltpu.VMEM(b_in.shape, bf16),
            pltpu.VMEM(w_out.shape[1:], bf16),
            pltpu.VMEM(b_out.shape, bf16),
            pltpu.VMEM((n_ex * pitch, LANES), f32),
            pltpu.VMEM((n * pitch, LANES), f32),
            pltpu.VMEM((n_ex, pitch, LANES), bf16),
            pltpu.VMEM((n, pitch, LANES), bf16),
            pltpu.VMEM((n, pitch, LANES), bf16),
            pltpu.VMEM((n, pitch, LANES), bf16),
            pltpu.VMEM((n, width), bf16),
            pltpu.VMEM((n, half), bf16),
            pltpu.VMEM((n_ex, m), bf16),
            pltpu.VMEM((n_ex, width), bf16),
            pltpu.SemaphoreType.DMA((4,)),
            pltpu.SemaphoreType.DMA((4,)),
            pltpu.SemaphoreType.DMA((4,)),
            pltpu.SemaphoreType.DMA((2,)),
            pltpu.SemaphoreType.DMA((2,)),
        ],
        compiler_params=pltpu.CompilerParams(
            collective_id=0, has_side_effects=True, vmem_limit_bytes=60 * 1024 * 1024
        ),
    )(tokens, router.T, w_in, b_in, w_out, b_out)


def solution(mesh):
    return jax.shard_map(
        functools.partial(shards, mesh.shape["dp"], mesh.shape["expert"]),
        mesh=mesh,
        in_specs=(
            P(("dp", "expert"), None, None),
            P(),
            P("expert", None, "dp"),
            P("expert", None),
            P("expert", "dp", None),
            P("expert", None),
        ),
        out_specs=P(("dp", "expert"), None, None),
        check_vma=False,
    )
```

```python
import functools

import jax
import jax.numpy as jnp
from jax import lax
from jax.experimental import pallas as pl
from jax.experimental.pallas import tpu as pltpu
from jax.sharding import PartitionSpec as P

MESH = pl.DeviceIdType.MESH
LANES = 128
SUBLANES = 16


def gelu(v):
    return v * (1.0 + lax.erf(v * (0.5**0.5))) * 0.5


def visit(n_dp, n_ex, me_dp, me_ex, action):
    half = n_ex // 2
    side = me_ex // half
    inner = lax.rem(me_ex, half)
    mirror = half - 1 - inner
    crossing = (1 - side) * half
    home = side * half

    def run(count, step):
        if count <= 8:
            for j in range(count):
                step(j)
        else:
            lax.fori_loop(0, count, lambda j, carry: step(j) or carry, 0)

    def far(j):
        for a in range(n_dp - 1, -1, -1):
            action(lax.rem(me_dp + a, n_dp), crossing + lax.rem(mirror - j + half, half))

    def near(j):
        for a in range(n_dp - 1, -1, -1):
            action(lax.rem(me_dp + a, n_dp), home + lax.rem(inner + 1 + j, half))

    run(half, far)
    run(half - 1, near)
    for a in range(n_dp - 1, 0, -1):
        action(lax.rem(me_dp + a, n_dp), me_ex)


def exchange(n_dp, n_ex, me_dp, me_ex, source, row_of, landing, send_sem, recv_sem, chunks):
    me = me_dp * n_ex + me_ex

    def send(a, e):
        pltpu.make_async_remote_copy(
            src_ref=source.at[row_of(a, e), pl.ds(0, chunks)],
            dst_ref=landing.at[me, pl.ds(0, chunks)],
            send_sem=send_sem,
            recv_sem=recv_sem,
            device_id=(a, e),
            device_id_type=MESH,
        ).start()

    visit(n_dp, n_ex, me_dp, me_ex, send)
    landing[me] = source[row_of(me_dp, me_ex)]


def wait_bytes(buffer, count, chunks, sem):
    rows = buffer.at[pl.ds(0, count), pl.ds(0, chunks)]
    pltpu.make_async_copy(rows, rows, sem).wait()


def kernel(
    n_dp,
    n_ex,
    tokens_hbm,
    router_hbm,
    w_in_hbm,
    b_in_hbm,
    w_out_hbm,
    b_out_hbm,
    comb_ref,
    eo,
    tok,
    router,
    w_in,
    b_in,
    w_out,
    b_out,
    wide_slots,
    wide_rows,
    send1,
    recv1,
    send2,
    recv2,
    x_ref,
    hid,
    load_sems,
    w_in_sems,
    w_out_sems,
    send_sems,
    recv_sems,
):
    n = n_dp * n_ex
    me_dp = lax.axis_index("dp")
    me_ex = lax.axis_index("expert")
    width = tok.shape[1]
    chunks = width // LANES
    pitch = send1.shape[1]

    loads = [
        pltpu.make_async_copy(tokens_hbm.at[0], tok, load_sems.at[0]),
        pltpu.make_async_copy(router_hbm, router, load_sems.at[1]),
        pltpu.make_async_copy(b_in_hbm, b_in, load_sems.at[2]),
        pltpu.make_async_copy(b_out_hbm, b_out, load_sems.at[3]),
    ]
    loads[0].start()
    loads[1].start()
    barrier = pltpu.get_barrier_semaphore()

    def greet(a, e):
        pl.semaphore_signal(barrier, inc=1, device_id=(a, e), device_id_type=MESH)

    visit(n_dp, n_ex, me_dp, me_ex, greet)

    def pieces(hbm, vmem, sems):
        count = sems.shape[0]
        rows = vmem.shape[0] // count
        return [
            pltpu.make_async_copy(
                hbm.at[0, pl.ds(i * rows, rows)], vmem.at[pl.ds(i * rows, rows)], sems.at[i]
            )
            for i in range(count)
        ]

    w_in_loads = pieces(w_in_hbm, w_in, w_in_sems)
    w_out_loads = pieces(w_out_hbm, w_out, w_out_sems)
    for load in w_in_loads + loads[2:] + w_out_loads:
        load.start()

    loads[0].wait()
    loads[1].wait()
    logits = lax.dot_general(
        router[...], tok[...], (((1,), (1,)), ((), ())), preferred_element_type=jnp.float32
    )
    over_tokens = jnp.exp(logits - jnp.max(logits, axis=1, keepdims=True))
    dispatch = (over_tokens / jnp.sum(over_tokens, axis=1, keepdims=True)).astype(jnp.bfloat16)
    slots = jnp.dot(dispatch, tok[...], preferred_element_type=jnp.float32)
    for j in range(chunks):
        wide_slots[pl.ds(j, n_ex, stride=pitch), :] = slots[:, j * LANES : (j + 1) * LANES]
    send1[...] = wide_slots[...].reshape(send1.shape).astype(jnp.bfloat16)

    pl.semaphore_wait(barrier, n - 1)
    exchange(
        n_dp, n_ex, me_dp, me_ex, send1, lambda a, e: e, recv1, send_sems.at[0], recv_sems.at[0], chunks
    )

    over_experts = jnp.exp(logits - jnp.max(logits, axis=0, keepdims=True))
    combine = over_experts / jnp.sum(over_experts, axis=0, keepdims=True)
    comb_ref[...] = combine.astype(jnp.bfloat16)

    for load in loads[2:] + w_in_loads:
        load.wait()
    wait_bytes(recv1, n - 1, chunks, recv_sems.at[0])
    wide_rows[...] = recv1[...].astype(jnp.float32).reshape(wide_rows.shape)
    for j in range(chunks):
        x_ref[:, j * LANES : (j + 1) * LANES] = wide_rows[pl.ds(j, n, stride=pitch), :].astype(jnp.bfloat16)

    half = w_in.shape[1]
    tile = 2 * LANES

    for at in range(0, half, tile):
        bias = b_in[:, pl.ds(pl.multiple_of(me_dp * half + at, LANES), tile)].astype(jnp.float32)
        v = jnp.dot(x_ref[...], w_in[:, at : at + tile], preferred_element_type=jnp.float32) + bias
        hid[:, at : at + tile] = gelu(v).astype(jnp.bfloat16)

    for load in w_out_loads:
        load.wait()
    keep = (me_dp == 0).astype(jnp.float32)
    for at in range(0, width, tile):
        y = jnp.dot(hid[...], w_out[:, at : at + tile], preferred_element_type=jnp.float32)
        y = y + keep * b_out[:, at : at + tile].astype(jnp.float32)
        for c in range(tile // LANES):
            wide_rows[pl.ds(at // LANES + c, n, stride=pitch), :] = y[:, c * LANES : (c + 1) * LANES]
    send2[...] = wide_rows[...].reshape(send2.shape).astype(jnp.bfloat16)

    exchange(
        n_dp, n_ex, me_dp, me_ex, send2, lambda a, e: a * n_ex + e, recv2, send_sems.at[1], recv_sems.at[1], chunks
    )
    wait_bytes(recv2, n - 1, chunks, recv_sems.at[1])
    wide_rows[...] = recv2[...].astype(jnp.float32).reshape(wide_rows.shape)
    for j in range(chunks):
        total = wide_rows[pl.ds(j, n_ex, stride=pitch), :]
        for a in range(1, n_dp):
            total = total + wide_rows[pl.ds(a * n_ex * pitch + j, n_ex, stride=pitch), :]
        eo[:, j * LANES : (j + 1) * LANES] = total.astype(jnp.bfloat16)
    wait_bytes(recv1, n - 1, chunks, send_sems.at[0])
    wait_bytes(recv2, n - 1, chunks, send_sems.at[1])


def mix_kernel(combine, expert_out, out_hbm, mixed, sems):
    count = sems.shape[0]
    tile = mixed.shape[1] // count
    writes = []
    for i in range(count):
        columns = pl.ds(i * tile, tile)
        mixed[:, columns] = lax.dot_general(
            combine[...], expert_out[:, columns], (((0,), (0,)), ((), ())), preferred_element_type=jnp.float32
        ).astype(mixed.dtype)
        write = pltpu.make_async_copy(mixed.at[:, columns], out_hbm.at[0, :, columns], sems.at[i])
        write.start()
        writes.append(write)
    for write in writes:
        write.wait()


def shards(n_dp, n_ex, tokens, router, w_in, b_in, w_out, b_out):
    n = n_dp * n_ex
    images, m, width = tokens.shape
    assert images == 1 and w_in.shape[0] == 1
    half = w_in.shape[2]
    chunks = width // LANES
    pitch = -(-chunks // SUBLANES) * SUBLANES
    bf16, f32 = jnp.bfloat16, jnp.float32
    combine, expert_out = pl.pallas_call(
        functools.partial(kernel, n_dp, n_ex),
        out_shape=[
            pltpu.VMEM((n_ex, m), bf16),
            pltpu.VMEM((n_ex, width), bf16),
        ],
        in_specs=[pl.BlockSpec(memory_space=pltpu.HBM)] * 6,
        out_specs=[pl.BlockSpec(memory_space=pltpu.VMEM)] * 2,
        scratch_shapes=[
            pltpu.VMEM((m, width), bf16),
            pltpu.VMEM(router.shape[::-1], bf16),
            pltpu.VMEM(w_in.shape[1:], bf16),
            pltpu.VMEM(b_in.shape, bf16),
            pltpu.VMEM(w_out.shape[1:], bf16),
            pltpu.VMEM(b_out.shape, bf16),
            pltpu.VMEM((n_ex * pitch, LANES), f32),
            pltpu.VMEM((n * pitch, LANES), f32),
            pltpu.VMEM((n_ex, pitch, LANES), bf16),
            pltpu.VMEM((n, pitch, LANES), bf16),
            pltpu.VMEM((n, pitch, LANES), bf16),
            pltpu.VMEM((n, pitch, LANES), bf16),
            pltpu.VMEM((n, width), bf16),
            pltpu.VMEM((n, half), bf16),
            pltpu.SemaphoreType.DMA((4,)),
            pltpu.SemaphoreType.DMA((4,)),
            pltpu.SemaphoreType.DMA((4,)),
            pltpu.SemaphoreType.DMA((2,)),
            pltpu.SemaphoreType.DMA((2,)),
        ],
        compiler_params=pltpu.CompilerParams(
            collective_id=0, has_side_effects=True, vmem_limit_bytes=60 * 1024 * 1024
        ),
    )(tokens, router.T, w_in, b_in, w_out, b_out)
    tile = 2 * LANES
    return pl.pallas_call(
        mix_kernel,
        out_shape=jax.ShapeDtypeStruct(tokens.shape, bf16),
        in_specs=[pl.BlockSpec(memory_space=pltpu.VMEM)] * 2,
        out_specs=pl.BlockSpec(memory_space=pltpu.HBM),
        scratch_shapes=[
            pltpu.VMEM((m, width), bf16),
            pltpu.SemaphoreType.DMA((width // tile,)),
        ],
        compiler_params=pltpu.CompilerParams(vmem_limit_bytes=8 * 1024 * 1024),
    )(combine, expert_out)


def solution(mesh):
    return jax.shard_map(
        functools.partial(shards, mesh.shape["dp"], mesh.shape["expert"]),
        mesh=mesh,
        in_specs=(
            P(("dp", "expert"), None, None),
            P(),
            P("expert", None, "dp"),
            P("expert", None),
            P("expert", "dp", None),
            P("expert", None),
        ),
        out_specs=P(("dp", "expert"), None, None),
        check_vma=False,
    )
```

```python
import functools

import jax
import jax.numpy as jnp
from jax import lax
from jax.experimental import pallas as pl
from jax.experimental.pallas import tpu as pltpu
from jax.sharding import PartitionSpec as P

MESH = pl.DeviceIdType.MESH
LANES = 128
SUBLANES = 16


def gelu(v):
    return v * (1.0 + lax.erf(v * (0.5**0.5))) * 0.5


def visit(n_dp, n_ex, me_dp, me_ex, action):
    half = n_ex // 2
    side = me_ex // half
    inner = lax.rem(me_ex, half)
    mirror = half - 1 - inner
    crossing = (1 - side) * half
    home = side * half

    def run(count, step):
        if count <= 8:
            for j in range(count):
                step(j)
        else:
            lax.fori_loop(0, count, lambda j, carry: step(j) or carry, 0)

    def far(j):
        for a in range(n_dp - 1, -1, -1):
            action(lax.rem(me_dp + a, n_dp), crossing + lax.rem(mirror - j + half, half))

    def near(j):
        for a in range(n_dp - 1, -1, -1):
            action(lax.rem(me_dp + a, n_dp), home + lax.rem(inner + 1 + j, half))

    run(half, far)
    run(half - 1, near)
    for a in range(n_dp - 1, 0, -1):
        action(lax.rem(me_dp + a, n_dp), me_ex)


def exchange(n_dp, n_ex, me_dp, me_ex, source, row_of, landing, send_sem, recv_sem, chunks):
    me = me_dp * n_ex + me_ex

    def send(a, e):
        pltpu.make_async_remote_copy(
            src_ref=source.at[row_of(a, e), pl.ds(0, chunks)],
            dst_ref=landing.at[me, pl.ds(0, chunks)],
            send_sem=send_sem,
            recv_sem=recv_sem,
            device_id=(a, e),
            device_id_type=MESH,
        ).start()

    visit(n_dp, n_ex, me_dp, me_ex, send)
    landing[me] = source[row_of(me_dp, me_ex)]


def wait_bytes(buffer, count, chunks, sem):
    rows = buffer.at[pl.ds(0, count), pl.ds(0, chunks)]
    pltpu.make_async_copy(rows, rows, sem).wait()


def kernel(
    n_dp,
    n_ex,
    tokens_hbm,
    router_hbm,
    w_in_hbm,
    b_in_hbm,
    w_out_hbm,
    b_out_hbm,
    comb_ref,
    eo,
    tok,
    router,
    w_in,
    b_in,
    w_out,
    b_out,
    wide_slots,
    wide_rows,
    send1,
    recv1,
    send2,
    recv2,
    x_ref,
    hid,
    load_sems,
    w_in_sems,
    w_out_sems,
    send_sems,
    recv_sems,
):
    n = n_dp * n_ex
    me_dp = lax.axis_index("dp")
    me_ex = lax.axis_index("expert")
    width = tok.shape[1]
    chunks = width // LANES
    pitch = send1.shape[1]

    loads = [
        pltpu.make_async_copy(tokens_hbm.at[0], tok, load_sems.at[0]),
        pltpu.make_async_copy(router_hbm, router, load_sems.at[1]),
        pltpu.make_async_copy(b_in_hbm, b_in, load_sems.at[2]),
        pltpu.make_async_copy(b_out_hbm, b_out, load_sems.at[3]),
    ]
    loads[0].start()
    loads[1].start()
    barrier = pltpu.get_barrier_semaphore()

    def greet(a, e):
        pl.semaphore_signal(barrier, inc=1, device_id=(a, e), device_id_type=MESH)

    visit(n_dp, n_ex, me_dp, me_ex, greet)

    def pieces(hbm, vmem, sems):
        count = sems.shape[0]
        rows = vmem.shape[0] // count
        return [
            pltpu.make_async_copy(
                hbm.at[0, pl.ds(i * rows, rows)], vmem.at[pl.ds(i * rows, rows)], sems.at[i]
            )
            for i in range(count)
        ]

    w_in_loads = pieces(w_in_hbm, w_in, w_in_sems)
    w_out_loads = pieces(w_out_hbm, w_out, w_out_sems)
    for load in w_in_loads + loads[2:] + w_out_loads:
        load.start()

    loads[0].wait()
    loads[1].wait()
    logits = lax.dot_general(
        router[...], tok[...], (((1,), (1,)), ((), ())), preferred_element_type=jnp.float32
    )
    over_tokens = jnp.exp(logits - jnp.max(logits, axis=1, keepdims=True))
    dispatch = (over_tokens / jnp.sum(over_tokens, axis=1, keepdims=True)).astype(jnp.bfloat16)
    slots = jnp.dot(dispatch, tok[...], preferred_element_type=jnp.float32)
    for j in range(chunks):
        wide_slots[pl.ds(j, n_ex, stride=pitch), :] = slots[:, j * LANES : (j + 1) * LANES]
    send1[...] = wide_slots[...].reshape(send1.shape).astype(jnp.bfloat16)

    pl.semaphore_wait(barrier, n - 1)
    exchange(
        n_dp, n_ex, me_dp, me_ex, send1, lambda a, e: e, recv1, send_sems.at[0], recv_sems.at[0], chunks
    )

    over_experts = jnp.exp(logits - jnp.max(logits, axis=0, keepdims=True))
    combine = over_experts / jnp.sum(over_experts, axis=0, keepdims=True)
    comb_ref[...] = combine.T.astype(jnp.bfloat16)

    for load in loads[2:] + w_in_loads:
        load.wait()
    wait_bytes(recv1, n - 1, chunks, recv_sems.at[0])
    wide_rows[...] = recv1[...].astype(jnp.float32).reshape(wide_rows.shape)
    for j in range(chunks):
        x_ref[:, j * LANES : (j + 1) * LANES] = wide_rows[pl.ds(j, n, stride=pitch), :].astype(jnp.bfloat16)

    half = w_in.shape[1]
    tile = 2 * LANES

    for at in range(0, half, tile):
        bias = b_in[:, pl.ds(pl.multiple_of(me_dp * half + at, LANES), tile)].astype(jnp.float32)
        v = jnp.dot(x_ref[...], w_in[:, at : at + tile], preferred_element_type=jnp.float32) + bias
        hid[:, at : at + tile] = gelu(v).astype(jnp.bfloat16)

    for load in w_out_loads:
        load.wait()
    keep = (me_dp == 0).astype(jnp.float32)
    for at in range(0, width, tile):
        y = jnp.dot(hid[...], w_out[:, at : at + tile], preferred_element_type=jnp.float32)
        y = y + keep * b_out[:, at : at + tile].astype(jnp.float32)
        for c in range(tile // LANES):
            wide_rows[pl.ds(at // LANES + c, n, stride=pitch), :] = y[:, c * LANES : (c + 1) * LANES]
    send2[...] = wide_rows[...].reshape(send2.shape).astype(jnp.bfloat16)

    exchange(
        n_dp, n_ex, me_dp, me_ex, send2, lambda a, e: a * n_ex + e, recv2, send_sems.at[1], recv_sems.at[1], chunks
    )
    wait_bytes(recv2, n - 1, chunks, recv_sems.at[1])
    wide_rows[...] = recv2[...].astype(jnp.float32).reshape(wide_rows.shape)
    for j in range(chunks):
        total = wide_rows[pl.ds(j, n_ex, stride=pitch), :]
        for a in range(1, n_dp):
            total = total + wide_rows[pl.ds(a * n_ex * pitch + j, n_ex, stride=pitch), :]
        eo[:, j * LANES : (j + 1) * LANES] = total.astype(jnp.bfloat16)
    wait_bytes(recv1, n - 1, chunks, send_sems.at[0])
    wait_bytes(recv2, n - 1, chunks, send_sems.at[1])


def mix_kernel(combine, expert_out, out_hbm, mixed, sems):
    count = sems.shape[0]
    tile = mixed.shape[1] // count
    writes = []
    for i in range(count):
        columns = pl.ds(i * tile, tile)
        mixed[:, columns] = jnp.dot(
            combine[...], expert_out[:, columns], preferred_element_type=jnp.float32
        ).astype(mixed.dtype)
        write = pltpu.make_async_copy(mixed.at[:, columns], out_hbm.at[0, :, columns], sems.at[i])
        write.start()
        writes.append(write)
    for write in writes:
        write.wait()


def shards(n_dp, n_ex, tokens, router, w_in, b_in, w_out, b_out):
    n = n_dp * n_ex
    images, m, width = tokens.shape
    assert images == 1 and w_in.shape[0] == 1
    half = w_in.shape[2]
    chunks = width // LANES
    pitch = -(-chunks // SUBLANES) * SUBLANES
    bf16, f32 = jnp.bfloat16, jnp.float32
    combine, expert_out = pl.pallas_call(
        functools.partial(kernel, n_dp, n_ex),
        out_shape=[
            pltpu.VMEM((m, n_ex), bf16),
            pltpu.VMEM((n_ex, width), bf16),
        ],
        in_specs=[pl.BlockSpec(memory_space=pltpu.HBM)] * 6,
        out_specs=[pl.BlockSpec(memory_space=pltpu.VMEM)] * 2,
        scratch_shapes=[
            pltpu.VMEM((m, width), bf16),
            pltpu.VMEM(router.shape[::-1], bf16),
            pltpu.VMEM(w_in.shape[1:], bf16),
            pltpu.VMEM(b_in.shape, bf16),
            pltpu.VMEM(w_out.shape[1:], bf16),
            pltpu.VMEM(b_out.shape, bf16),
            pltpu.VMEM((n_ex * pitch, LANES), f32),
            pltpu.VMEM((n * pitch, LANES), f32),
            pltpu.VMEM((n_ex, pitch, LANES), bf16),
            pltpu.VMEM((n, pitch, LANES), bf16),
            pltpu.VMEM((n, pitch, LANES), bf16),
            pltpu.VMEM((n, pitch, LANES), bf16),
            pltpu.VMEM((n, width), bf16),
            pltpu.VMEM((n, half), bf16),
            pltpu.SemaphoreType.DMA((4,)),
            pltpu.SemaphoreType.DMA((4,)),
            pltpu.SemaphoreType.DMA((4,)),
            pltpu.SemaphoreType.DMA((2,)),
            pltpu.SemaphoreType.DMA((2,)),
        ],
        compiler_params=pltpu.CompilerParams(
            collective_id=0, has_side_effects=True, vmem_limit_bytes=60 * 1024 * 1024
        ),
    )(tokens, router.T, w_in, b_in, w_out, b_out)
    tile = 2 * LANES
    return pl.pallas_call(
        mix_kernel,
        out_shape=jax.ShapeDtypeStruct(tokens.shape, bf16),
        in_specs=[pl.BlockSpec(memory_space=pltpu.VMEM)] * 2,
        out_specs=pl.BlockSpec(memory_space=pltpu.HBM),
        scratch_shapes=[
            pltpu.VMEM((m, width), bf16),
            pltpu.SemaphoreType.DMA((width // tile,)),
        ],
        compiler_params=pltpu.CompilerParams(vmem_limit_bytes=8 * 1024 * 1024),
    )(combine, expert_out)


def solution(mesh):
    return jax.shard_map(
        functools.partial(shards, mesh.shape["dp"], mesh.shape["expert"]),
        mesh=mesh,
        in_specs=(
            P(("dp", "expert"), None, None),
            P(),
            P("expert", None, "dp"),
            P("expert", None),
            P("expert", "dp", None),
            P("expert", None),
        ),
        out_specs=P(("dp", "expert"), None, None),
        check_vma=False,
    )
```
